64 devices in a mesh: rep: 8 (over x, y, core), dp: 8 (over z).
Axes of the slice: x: 2, y: 2, z: 8, core: 2. Of those that a mesh axis runs over, the one named last changes fastest.
The devices are a block of a 4x4x8 slice.
Arguments:
- g_w_gate: bfloat16 [64, 2, 512, 4096], P(('rep', 'dp')), parts along dimension 0
- g_w_up: bfloat16 [64, 2, 512, 4096], P(('rep', 'dp')), parts along dimension 0
- g_w_down: bfloat16 [64, 2, 4096, 512], P(('rep', 'dp')), parts along dimension 0
- w_gate: bfloat16 [2, 512, 4096], replicated
- w_up: bfloat16 [2, 512, 4096], replicated
- w_down: bfloat16 [2, 4096, 512], replicated
- m_w_gate: float32 [2, 512, 4096], P(None, 'dp')
- m_w_up: float32 [2, 512, 4096], P(None, 'dp')
- m_w_down: float32 [2, 4096, 512], P(None, 'dp')
- v_w_gate: float32 [2, 512, 4096], P(None, 'dp')
- v_w_up: float32 [2, 512, 4096], P(None, 'dp')
- v_w_down: float32 [2, 4096, 512], P(None, 'dp')
Outputs:
- output 1: bfloat16 [16, 512, 4096], P('rep'), parts along dimension 0
- output 2: bfloat16 [16, 512, 4096], P('rep'), parts along dimension 0
- output 3: bfloat16 [16, 4096, 512], P('rep'), parts along dimension 0
- output 4: float32 [16, 512, 4096], P('rep', 'dp'), parts along dimension 0
- output 5: float32 [16, 512, 4096], P('rep', 'dp'), parts along dimension 0
- output 6: float32 [16, 4096, 512], P('rep', 'dp'), parts along dimension 0
- output 7: float32 [16, 512, 4096], P('rep', 'dp'), parts along dimension 0
- output 8: float32 [16, 512, 4096], P('rep', 'dp'), parts along dimension 0
- output 9: float32 [16, 4096, 512], P('rep', 'dp'), parts along dimension 0
There are 8 independent parts. The reference program is written for one: setup_inputs(seed, part) draws one part's arguments, and reference() takes and returns one part's arrays. A program takes and returns all parts, laid end to end along the dimension named above; an argument that names none is the same for every part.
All inputs are finite; a program needn't handle non-finite values.
Results may differ from the reference program's by a relative error of at most 0.022.
Values are sent between devices in bfloat16 or wider.
A program may use at most 768 MiB of HBM per device.

```python
import jax
import jax.numpy as jnp
from jax import lax

DEVICES = 8
D = 512
FF = 4096
LAYERS = 2
NAMES = ("w_gate", "w_up", "w_down")
SHAPES = {"w_gate": (LAYERS, D, FF), "w_up": (LAYERS, D, FF), "w_down": (LAYERS, FF, D)}


def setup_inputs(seed: int = 0, part: int = 0) -> dict:
    kz, *keys = jax.random.split(jax.random.key(seed), 1 + 5 * len(NAMES))
    loud = 2.0 ** jax.random.uniform(kz, (), jnp.float32, -1.0, 1.0)
    drawn = {}
    for name, key, both in zip(NAMES, keys[:3], keys[3:6], strict=True):
        own = jax.random.normal(jax.random.fold_in(key, part), (DEVICES, *SHAPES[name]), jnp.float32)
        shared = jax.random.normal(jax.random.fold_in(both, part), SHAPES[name], jnp.float32)
        drawn["g_" + name] = (loud * (0.7 * shared / DEVICES + 0.7 * own * DEVICES**-0.5)).astype(jnp.bfloat16)
    for name, key in zip(NAMES, keys[6:9], strict=True):
        drawn[name] = (jax.random.normal(key, SHAPES[name], jnp.float32) * SHAPES[name][1] ** -0.5).astype(jnp.bfloat16)
    for name, key in zip(NAMES, keys[9:12], strict=True):
        drawn["m_" + name] = loud * 0.5 * jax.random.normal(key, SHAPES[name], jnp.float32)
    for name, key in zip(NAMES, keys[12:15], strict=True):
        drawn["v_" + name] = loud * loud * jax.random.uniform(key, SHAPES[name], jnp.float32, 0.5, 1.5)
    return drawn


def adamw(w, m, v, g):
    m = 0.9 * m + 0.1 * g
    v = 0.95 * v + 0.05 * g * g
    step = m * lax.rsqrt(v + 1e-8) + 0.1 * w
    return (w - 0.02 * step).astype(jnp.bfloat16), m, v


def reference(g_w_gate, g_w_up, g_w_down, w_gate, w_up, w_down, m_w_gate, m_w_up, m_w_down, v_w_gate, v_w_up, v_w_down):
    def total(terms):
        return lax.scan(lambda so_far, term: (so_far + term.astype(jnp.float32), None), jnp.zeros(terms.shape[1:], jnp.float32), terms)[0]

    gradients = [total(terms).astype(jnp.bfloat16).astype(jnp.float32) for terms in (g_w_gate, g_w_up, g_w_down)]
    new = [
        adamw(w.astype(jnp.float32), m, v, g)
        for w, m, v, g in zip((w_gate, w_up, w_down), (m_w_gate, m_w_up, m_w_down), (v_w_gate, v_w_up, v_w_down), gradients, strict=True)
    ]
    return tuple(one[which] for which in range(3) for one in new)
```

```python
import jax
import jax.numpy as jnp
from jax import lax
from jax.sharding import PartitionSpec as P


def adamw(w, m, v, g):
    m = 0.9 * m + 0.1 * g
    v = 0.95 * v + 0.05 * g * g
    step = m * lax.rsqrt(v + 1e-8) + 0.1 * w
    return (w - 0.02 * step).astype(jnp.bfloat16), m, v


def solution(mesh):
    n = mesh.shape["dp"]
    perms = [[(d, (d + 1) % n) for d in range(n)], [(d, (d - 1) % n) for d in range(n)]]

    def step(*arrays):
        terms, weights, m, v = (arrays[i : i + 3] for i in (0, 3, 6, 9))
        terms = [t[0] for t in terms]
        me = lax.axis_index("dp")
        f32, bf16 = jnp.float32, jnp.bfloat16

        def behind(way, hops):
            return (me + n - hops) % n if way == 0 else (me + hops) % n

        def block(x, i, way, owner):
            half = m[i].shape[1] // 2
            return lax.dynamic_slice_in_dim(x, owner * 2 * half + way * half, half, 1)

        pieces = [(i, way) for i in range(3) for way in range(2)]
        moving = {p: block(terms[p[0]], *p, behind(p[1], 1)) for p in pieces}
        for s in range(n - 1):
            for p in pieces:
                got = lax.ppermute(moving[p], "dp", perms[p[1]])
                moving[p] = (got.astype(f32) + block(terms[p[0]], *p, behind(p[1], s + 2)).astype(f32)).astype(bf16)
        new = {}
        outs = [jnp.zeros(w.shape, bf16) for w in weights]
        for i, way in pieces:
            half = m[i].shape[1] // 2
            mine = lambda x: lax.slice_in_dim(x, way * half, way * half + half, axis=1)
            new[i, way] = adamw(block(weights[i], i, way, me).astype(f32), mine(m[i]), mine(v[i]), moving[i, way].astype(f32))
            moving[i, way] = new[i, way][0]

        def put(i, way, owner, x):
            half = m[i].shape[1] // 2
            outs[i] = lax.dynamic_update_slice_in_dim(outs[i], x, owner * 2 * half + way * half, 1)

        for p in pieces:
            put(*p, me, moving[p])
        for s in range(n - 1):
            for p in pieces:
                moving[p] = lax.ppermute(moving[p], "dp", perms[p[1]])
                put(*p, behind(p[1], s + 1), moving[p])
        ms = [jnp.concatenate([new[i, 0][1], new[i, 1][1]], 1) for i in range(3)]
        vs = [jnp.concatenate([new[i, 0][2], new[i, 1][2]], 1) for i in range(3)]
        return (*outs, *ms, *vs)

    all_of, cut = P(None, None, None), P(None, "dp", None)
    return jax.shard_map(
        step,
        mesh=mesh,
        in_specs=(P(("rep", "dp"), None, None, None),) * 3 + (all_of,) * 3 + (cut,) * 6,
        out_specs=(P("rep", None, None),) * 3 + (P("rep", "dp", None),) * 6,
        check_vma=False,
    )
```

```python
import jax
import jax.numpy as jnp
from jax import lax
from jax.experimental import pallas as pl
from jax.experimental.pallas import tpu as pltpu
from jax.sharding import PartitionSpec as P


def adamw(w, m, v, g):
    m = 0.9 * m + 0.1 * g
    v = 0.95 * v + 0.05 * g * g
    step = m * lax.rsqrt(v + 1e-8) + 0.1 * w
    return (w - 0.02 * step).astype(jnp.bfloat16), m, v


def blank(shape, dtype):
    return pl.pallas_call(
        lambda out: None,
        out_shape=jax.ShapeDtypeStruct(shape, dtype),
        out_specs=pl.BlockSpec(memory_space=pltpu.HBM),
        name="blank",
    )()


def in_hbm(x):
    return pl.pallas_call(
        lambda x, out: None,
        out_shape=jax.ShapeDtypeStruct(x.shape, x.dtype),
        in_specs=[pl.BlockSpec(memory_space=pltpu.HBM)],
        out_specs=pl.BlockSpec(memory_space=pltpu.HBM),
        input_output_aliases={0: 0},
        name="in_hbm",
    )(x)


def solution(mesh):
    n = mesh.shape["dp"]
    perms = [[(d, (d + 1) % n) for d in range(n)], [(d, (d - 1) % n) for d in range(n)]]

    def step(*arrays):
        terms, weights, m, v = (arrays[i : i + 3] for i in (0, 3, 6, 9))
        terms = [t[0] for t in terms]
        me = lax.axis_index("dp")
        f32, bf16 = jnp.float32, jnp.bfloat16

        def behind(way, hops):
            return (me + n - hops) % n if way == 0 else (me + hops) % n

        def block(x, i, way, owner):
            half = m[i].shape[1] // 2
            return lax.dynamic_slice_in_dim(x, owner * 2 * half + way * half, half, 1)

        pieces = [(i, way) for i in range(3) for way in range(2)]
        moving = {p: block(terms[p[0]], *p, behind(p[1], 1)) for p in pieces}
        for s in range(n - 1):
            for p in pieces:
                got = lax.ppermute(moving[p], "dp", perms[p[1]])
                moving[p] = (got.astype(f32) + block(terms[p[0]], *p, behind(p[1], s + 2)).astype(f32)).astype(bf16)
        new = {}
        outs = [blank(w.shape, bf16) for w in weights]
        for i, way in pieces:
            half = m[i].shape[1] // 2
            mine = lambda x: lax.slice_in_dim(x, way * half, way * half + half, axis=1)
            new[i, way] = adamw(block(weights[i], i, way, me).astype(f32), mine(m[i]), mine(v[i]), moving[i, way].astype(f32))
            moving[i, way] = new[i, way][0]

        def put(i, way, owner, x):
            half = m[i].shape[1] // 2
            outs[i] = lax.dynamic_update_slice_in_dim(outs[i], x, owner * 2 * half + way * half, 1)

        for p in pieces:
            put(*p, me, moving[p])
        for s in range(n - 1):
            if s == n - 2:
                outs = [in_hbm(one) for one in outs]
            for p in pieces:
                moving[p] = lax.ppermute(moving[p], "dp", perms[p[1]])
                put(*p, behind(p[1], s + 1), moving[p])
        ms = [jnp.concatenate([new[i, 0][1], new[i, 1][1]], 1) for i in range(3)]
        vs = [jnp.concatenate([new[i, 0][2], new[i, 1][2]], 1) for i in range(3)]
        return (*outs, *ms, *vs)

    all_of, cut = P(None, None, None), P(None, "dp", None)
    return jax.shard_map(
        step,
        mesh=mesh,
        in_specs=(P(("rep", "dp"), None, None, None),) * 3 + (all_of,) * 3 + (cut,) * 6,
        out_specs=(P("rep", None, None),) * 3 + (P("rep", "dp", None),) * 6,
        check_vma=False,
    )
```

```python
import jax
import jax.numpy as jnp
from jax import lax
from jax.experimental import pallas as pl
from jax.experimental.pallas import tpu as pltpu
from jax.sharding import PartitionSpec as P


def adamw(w, m, v, g):
    m = 0.9 * m + 0.1 * g
    v = 0.95 * v + 0.05 * g * g
    step = m * lax.rsqrt(v + 1e-8) + 0.1 * w
    return (w - 0.02 * step).astype(jnp.bfloat16), m, v


def blank(shape, dtype):
    return pl.pallas_call(
        lambda out: None,
        out_shape=jax.ShapeDtypeStruct(shape, dtype),
        out_specs=pl.BlockSpec(memory_space=pltpu.HBM),
        name="blank",
    )()


SMALL = pltpu.CompilerParams(vmem_limit_bytes=1 << 20)
ANY = pl.BlockSpec(memory_space=pl.ANY)


def half_rows(n, half, way, hops):
    me = lax.axis_index("dp")
    owner = lax.rem(me + n - hops, n) if way == 0 else lax.rem(me + hops, n)
    return pl.ds(pl.multiple_of(owner * (2 * half) + way * half, half), half)


def place(n, whole, parts):
    half = parts[0].shape[1]

    def kernel(_, *refs):
        *came, out, done = refs
        copies = [
            pltpu.make_async_copy(part, out.at[:, half_rows(n, half, way, n - 1), :], done.at[way]) for way, part in enumerate(came)
        ]
        for copy in copies:
            copy.start()
        for copy in copies:
            copy.wait()

    return pl.pallas_call(
        kernel,
        out_shape=jax.ShapeDtypeStruct(whole.shape, whole.dtype),
        in_specs=[pl.BlockSpec(memory_space=pltpu.HBM), ANY, ANY],
        out_specs=pl.BlockSpec(memory_space=pltpu.HBM),
        scratch_shapes=[pltpu.SemaphoreType.DMA((2,))],
        input_output_aliases={0: 0},
        cost_estimate=pl.CostEstimate(flops=1 << 22, bytes_accessed=8 * parts[0].size, transcendentals=0),
        compiler_params=SMALL,
        name="place",
    )(whole, *parts)


def first_terms(n, term, half):
    def kernel(term, *refs):
        *outs, done = refs
        copies = [
            pltpu.make_async_copy(term.at[:, half_rows(n, half, way, 1), :], out, done.at[way]) for way, out in enumerate(outs)
        ]
        for copy in copies:
            copy.start()
        for copy in copies:
            copy.wait()

    return pl.pallas_call(
        kernel,
        out_shape=[jax.ShapeDtypeStruct((term.shape[0], half, term.shape[2]), term.dtype)] * 2,
        in_specs=[pl.BlockSpec(memory_space=pltpu.HBM)],
        out_specs=[ANY, ANY],
        scratch_shapes=[pltpu.SemaphoreType.DMA((2,))],
        cost_estimate=pl.CostEstimate(flops=1 << 22, bytes_accessed=4 * term.size // n, transcendentals=0),
        compiler_params=SMALL,
        name="first_terms",
    )(term)


def solution(mesh):
    n = mesh.shape["dp"]
    perms = [[(d, (d + 1) % n) for d in range(n)], [(d, (d - 1) % n) for d in range(n)]]

    def step(*arrays):
        terms, weights, m, v = (arrays[i : i + 3] for i in (0, 3, 6, 9))
        terms = [t[0] for t in terms]
        me = lax.axis_index("dp")
        f32, bf16 = jnp.float32, jnp.bfloat16

        def behind(way, hops):
            return (me + n - hops) % n if way == 0 else (me + hops) % n

        def block(x, i, way, owner):
            half = m[i].shape[1] // 2
            return lax.dynamic_slice_in_dim(x, owner * 2 * half + way * half, half, 1)

        pieces = [(i, way) for i in range(3) for way in range(2)]
        moving = {p: block(terms[p[0]], *p, behind(p[1], 1)) for p in pieces}
        for s in range(n - 1):
            for p in pieces:
                got = lax.ppermute(moving[p], "dp", perms[p[1]])
                moving[p] = (got.astype(f32) + block(terms[p[0]], *p, behind(p[1], s + 2)).astype(f32)).astype(bf16)
        new = {}
        outs = [blank(w.shape, bf16) for w in weights]
        for i, way in pieces:
            half = m[i].shape[1] // 2
            mine = lambda x: lax.slice_in_dim(x, way * half, way * half + half, axis=1)
            new[i, way] = adamw(block(weights[i], i, way, me).astype(f32), mine(m[i]), mine(v[i]), moving[i, way].astype(f32))
            moving[i, way] = new[i, way][0]

        def put(i, way, owner, x):
            half = m[i].shape[1] // 2
            outs[i] = lax.dynamic_update_slice_in_dim(outs[i], x, owner * 2 * half + way * half, 1)

        for p in pieces:
            put(*p, me, moving[p])
        for s in range(n - 1):
            for p in pieces:
                moving[p] = lax.ppermute(moving[p], "dp", perms[p[1]])
                if s < n - 2:
                    put(*p, behind(p[1], s + 1), moving[p])
        outs = [place(n, outs[i], [moving[i, way] for way in range(2)]) for i in range(3)]
        ms = [jnp.concatenate([new[i, 0][1], new[i, 1][1]], 1) for i in range(3)]
        vs = [jnp.concatenate([new[i, 0][2], new[i, 1][2]], 1) for i in range(3)]
        return (*outs, *ms, *vs)

    all_of, cut = P(None, None, None), P(None, "dp", None)
    return jax.shard_map(
        step,
        mesh=mesh,
        in_specs=(P(("rep", "dp"), None, None, None),) * 3 + (all_of,) * 3 + (cut,) * 6,
        out_specs=(P("rep", None, None),) * 3 + (P("rep", "dp", None),) * 6,
        check_vma=False,
    )
```

```python
import functools

import jax
import jax.numpy as jnp
from jax import lax
from jax.experimental import pallas as pl
from jax.experimental.pallas import tpu as pltpu
from jax.sharding import PartitionSpec as P

MESH = pl.DeviceIdType.MESH
ANY = pl.BlockSpec(memory_space=pl.ANY)
HBM = pl.BlockSpec(memory_space=pltpu.HBM)
TILE_ROWS, TILE_COLUMNS = 32, 512


def adamw(w, m, v, g):
    m = 0.9 * m + 0.1 * g
    v = 0.95 * v + 0.05 * g * g
    step = m * lax.rsqrt(v + 1e-8) + 0.1 * w
    return (w - 0.02 * step).astype(jnp.bfloat16), m, v


def behind(n, way, hops):
    me = lax.axis_index("dp")
    return lax.rem(me + n - hops, n) if way == 0 else lax.rem(me + hops, n)


def half_rows(n, half, way, hops):
    return pl.ds(pl.multiple_of(behind(n, way, hops) * (2 * half) + way * half, half), half)


def tiles(layers, rows, columns, body):
    high, wide = min(TILE_ROWS, rows), min(TILE_COLUMNS, columns)
    across, down = columns // wide, rows // high

    def one(t, _):
        body(t // (across * down), pl.ds((t // across) % down * high, high), pl.ds(pl.multiple_of((t % across) * wide, wide), wide))
        return 0

    lax.fori_loop(0, layers * down * across, one, 0)


def rings(n, count, *refs):
    g, w, m, v = (refs[i * count : (i + 1) * count] for i in range(4))
    w_new, m_new, v_new = (refs[(4 + i) * count : (5 + i) * count] for i in range(3))
    ends = [refs[7 * count + 2 * i : 7 * count + 2 * i + 2] for i in range(count)]
    rest = refs[9 * count :]
    sums, terms, w_own, m_own, v_own = (rest[i * count : (i + 1) * count] for i in range(5))
    sum_sent, sum_came, new_sent, new_came, term_sem, in_sem, out_sem = rest[5 * count :]

    layers = g[0].shape[0]
    pieces = [(i, way) for i in range(count) for way in range(2)]
    half = [one.shape[1] // 2 for one in m]
    ahead = [behind(n, 1 - way, 1) for way in range(2)]
    last = n - 2
    final = n - 3

    def rows(i, way, hops):
        return half_rows(n, half[i], way, hops)

    def own(i, way):
        return pl.ds(way * half[i], half[i])

    def term(i, way, step):
        slot = lax.rem(step, 2)
        return pltpu.make_async_copy(g[i].at[:, rows(i, way, step + 2), :], terms[i].at[slot, way], term_sem.at[slot, i, way])

    def remote(source, target, sent, came, way):
        return pltpu.make_async_remote_copy(
            src_ref=source, dst_ref=target, send_sem=sent, recv_sem=came, device_id={"dp": ahead[way]}, device_id_type=MESH
        )

    def send_sum(i, way, step, source):
        return remote(source, sums[i].at[step, way], sum_sent.at[step, i, way], sum_came.at[step, i, way], way)

    def first_sum(i, way):
        return send_sum(i, way, 0, g[i].at[:, rows(i, way, 1), :])

    def sum_at(i, way, step):
        return send_sum(i, way, step, sums[i].at[step, way])

    def send_new(i, way, step, source, target):
        return remote(source, target, new_sent.at[step, i, way], new_came.at[step, i, way], way)

    def first_new(i, way):
        return send_new(i, way, 0, w_own[i].at[:, own(i, way), :], w_new[i].at[:, rows(i, way, 0), :])

    def new_at(i, way, step, hops):
        where = w_new[i].at[:, rows(i, way, hops), :]
        return send_new(i, way, step, where, where)

    def end_at(i, way, hops):
        return send_new(i, way, final, w_new[i].at[:, rows(i, way, hops), :], ends[i][way])

    def into(i):
        mine = pl.ds(pl.multiple_of(behind(n, 0, 0) * (2 * half[i]), 2 * half[i]), 2 * half[i])
        return [
            pltpu.make_async_copy(w[i].at[:, mine, :], w_own[i], in_sem.at[0, i]),
            pltpu.make_async_copy(m[i], m_own[i], in_sem.at[1, i]),
            pltpu.make_async_copy(v[i], v_own[i], in_sem.at[2, i]),
        ]

    def out_of(i, way):
        here = own(i, way)
        return [
            pltpu.make_async_copy(w_own[i].at[:, here, :], w_new[i].at[:, rows(i, way, 0), :], out_sem.at[0, i, way]),
            pltpu.make_async_copy(m_own[i].at[:, here, :], m_new[i].at[:, here, :], out_sem.at[1, i, way]),
            pltpu.make_async_copy(v_own[i].at[:, here, :], v_new[i].at[:, here, :], out_sem.at[2, i, way]),
        ]

    barrier = pltpu.get_barrier_semaphore()
    for device in ahead:
        pl.semaphore_signal(barrier, inc=1, device_id={"dp": device}, device_id_type=MESH)
    pl.semaphore_wait(barrier, 2)

    def begin():
        for piece in pieces:
            first_sum(*piece).start()
        for step in range(2):
            for piece in pieces:
                term(*piece, step).start()

    later = lax.rem(lax.axis_index("rep"), 2) == 0
    first_in = into(0)

    @pl.when(jnp.logical_not(later))
    def _():
        begin()

    for copy in first_in:
        copy.start()

    @pl.when(later)
    def _():
        for copy in first_in:
            copy.wait()
        begin()

    for i in range(1, count):
        for copy in into(i):
            copy.start()

    def pass_on(step, _):
        slot = lax.rem(step, 2)
        for i, way in pieces:
            term(i, way, step).wait()
            sum_at(i, way, step).wait_recv()

            def add(layer, r, c):
                total = sums[i][step, way, layer, r, c].astype(jnp.float32) + terms[i][slot, way, layer, r, c].astype(jnp.float32)
                sums[i][step, way, layer, r, c] = total.astype(jnp.bfloat16)

            tiles(layers, half[i], m[i].shape[2], add)
            send_sum(i, way, step + 1, sums[i].at[step, way]).start()

            @pl.when(step + 2 < n - 1)
            def _():
                term(i, way, step + 2).start()

        return 0

    lax.fori_loop(0, last, pass_on, 0)

    @pl.when(jnp.logical_not(later))
    def _():
        for copy in first_in:
            copy.wait()

    for i in range(1, count):
        for copy in into(i):
            copy.wait()

    for i, way in pieces:
        term(i, way, last).wait()
        sum_at(i, way, last).wait_recv()

        def update(layer, r, c):
            total = sums[i][last, way, layer, r, c].astype(jnp.float32) + terms[i][last % 2, way, layer, r, c].astype(jnp.float32)
            gradient = total.astype(jnp.bfloat16).astype(jnp.float32)
            here = pl.ds(way * half[i] + r.start, r.size)
            new = adamw(w_own[i][layer, here, c].astype(jnp.float32), m_own[i][layer, here, c], v_own[i][layer, here, c], gradient)
            w_own[i][layer, here, c], m_own[i][layer, here, c], v_own[i][layer, here, c] = new

        tiles(layers, half[i], m[i].shape[2], update)
        first_new(i, way).start()
        for copy in out_of(i, way):
            copy.start()

    def hand_on(step, _):
        for i, way in pieces:
            new_at(i, way, step - 1, step).wait_recv()
            new_at(i, way, step, step).start()
        return 0

    lax.fori_loop(1, final, hand_on, 0)
    for i, way in pieces:
        new_at(i, way, final - 1, final).wait_recv()
        end_at(i, way, final).start()

    for piece in pieces:
        for copy in out_of(*piece):
            copy.wait()
        first_sum(*piece).wait_send()
        first_new(*piece).wait_send()

    def sums_sent(step, _):
        for piece in pieces:
            sum_at(*piece, step).wait_send()
        return 0

    def new_went(step, _):
        for piece in pieces:
            new_at(*piece, step, step).wait_send()
        return 0

    lax.fori_loop(1, n - 1, sums_sent, 0)
    lax.fori_loop(1, final, new_went, 0)
    for i, way in pieces:
        end_at(i, way, final).wait_send()
        end_at(i, way, final).wait_recv()


def ring_call(n, terms, weights, m, v):
    count, layers = len(m), weights[0].shape[0]
    halves = [(one.shape[1] // 2, one.shape[2]) for one in m]
    bf16, f32 = jnp.bfloat16, jnp.float32
    shape, semaphores, each = jax.ShapeDtypeStruct, pltpu.SemaphoreType.DMA, (count, 2)
    outs = pl.pallas_call(
        functools.partial(rings, n, count),
        out_shape=[
            *(shape(one.shape, bf16) for one in weights),
            *(shape(one.shape, f32) for one in m + v),
            *(shape((layers, *half), bf16) for half in halves for _ in range(2)),
        ],
        in_specs=[ANY] * (4 * count),
        out_specs=[ANY] * (5 * count),
        scratch_shapes=[
            *(pltpu.VMEM((n - 1, 2, layers, *half), bf16) for half in halves),
            *(pltpu.VMEM((2, 2, layers, *half), bf16) for half in halves),
            *(pltpu.VMEM(one.shape, bf16) for one in m),
            *(pltpu.VMEM(one.shape, f32) for one in m),
            *(pltpu.VMEM(one.shape, f32) for one in v),
            *(semaphores((n - 1, *each)) for _ in range(4)),
            semaphores((2, *each)),
            semaphores((3, count)),
            semaphores((3, *each)),
        ],
        compiler_params=pltpu.CompilerParams(collective_id=0, has_side_effects=True),
        name="rings",
    )(*terms, *weights, *m, *v)
    ends = [outs[3 * count + 2 * i : 3 * count + 2 * i + 2] for i in range(count)]
    return outs[:count], outs[count : 2 * count], outs[2 * count : 3 * count], ends


def copy_out(n, count, *refs):
    w, m, v = (refs[i * count : (i + 1) * count] for i in range(3))
    ends = [refs[3 * count + 2 * i : 3 * count + 2 * i + 2] for i in range(count)]
    w_out, m_out, v_out = (refs[(5 + i) * count : (6 + i) * count] for i in range(3))
    w_held, m_held, v_held = (refs[(8 + i) * count : (9 + i) * count] for i in range(3))
    came, went = refs[11 * count :]
    moves = []
    for i in range(count):
        half = m[i].shape[1] // 2
        for source, held, out in ((m[i], m_held[i], m_out[i]), (v[i], v_held[i], v_out[i])):
            moves += [(source.at[layer], held.at[layer], out.at[layer]) for layer in range(m[i].shape[0])]
        for hops in range(n - 1):
            for way in range(2):
                here = half_rows(n, half, way, hops)
                source = ends[i][way] if hops == n - 2 else w[i].at[:, here, :]
                moves.append((source, w_held[i].at[hops, way], w_out[i].at[:, here, :]))
    reads = [pltpu.make_async_copy(source, held, came.at[k]) for k, (source, held, _) in enumerate(moves)]
    writes = [pltpu.make_async_copy(held, out, went.at[k]) for k, (_, held, out) in enumerate(moves)]
    for read in reads:
        read.start()
    for read, write in zip(reads, writes, strict=True):
        read.wait()
        write.start()
    for write in writes:
        write.wait()


def copy_call(n, w, m, v, ends):
    count, layers = len(m), w[0].shape[0]
    halves = [(one.shape[1] // 2, one.shape[2]) for one in m]
    moves = count * (2 * layers + 2 * (n - 1))
    shape = jax.ShapeDtypeStruct
    size = 2 * sum(one.size * one.dtype.itemsize for one in (*w, *m, *v))
    outs = pl.pallas_call(
        functools.partial(copy_out, n, count),
        out_shape=[shape(one.shape, one.dtype) for one in (*w, *m, *v)],
        in_specs=[ANY] * (5 * count),
        out_specs=[ANY] * (3 * count),
        scratch_shapes=[
            *(pltpu.VMEM((n - 1, 2, layers, *half), jnp.bfloat16) for half in halves),
            *(pltpu.VMEM(one.shape, one.dtype) for one in (*m, *v)),
            pltpu.SemaphoreType.DMA((moves,)),
            pltpu.SemaphoreType.DMA((moves,)),
        ],
        cost_estimate=pl.CostEstimate(flops=1 << 26, bytes_accessed=size, transcendentals=0),
        name="copy_out",
    )(*w, *m, *v, *(end for pair in ends for end in pair))
    return outs[:count], outs[count : 2 * count], outs[2 * count :]


def place(n, whole, parts):
    half = parts[0].shape[1]

    def kernel(_, *refs):
        *came, out, done = refs
        copies = [
            pltpu.make_async_copy(part, out.at[:, half_rows(n, half, way, n - 1), :], done.at[way]) for way, part in enumerate(came)
        ]
        for copy in copies:
            copy.start()
        for copy in copies:
            copy.wait()

    return pl.pallas_call(
        kernel,
        out_shape=jax.ShapeDtypeStruct(whole.shape, whole.dtype),
        in_specs=[HBM, ANY, ANY],
        out_specs=HBM,
        scratch_shapes=[pltpu.SemaphoreType.DMA((2,))],
        input_output_aliases={0: 0},
        cost_estimate=pl.CostEstimate(flops=1 << 22, bytes_accessed=8 * parts[0].size, transcendentals=0),
        compiler_params=pltpu.CompilerParams(vmem_limit_bytes=1 << 20),
        name="place",
    )(whole, *parts)


def solution(mesh):
    n = mesh.shape["dp"]
    perms = [[(d, (d + 1) % n) for d in range(n)], [(d, (d - 1) % n) for d in range(n)]]

    def step(*arrays):
        count = len(arrays) // 4
        terms, weights, m, v = (list(arrays[i * count : (i + 1) * count]) for i in range(4))
        w_new, m_new, v_new, ends = ring_call(n, [one[0] for one in terms], weights, m, v)
        came = [[lax.ppermute(end, "dp", perms[way]) for way, end in enumerate(pair)] for pair in ends]
        w_new, m_new, v_new = copy_call(n, w_new, m_new, v_new, ends)
        w_new = [place(n, one, parts) for one, parts in zip(w_new, came, strict=True)]
        return (*w_new, *m_new, *v_new)

    all_of, cut = P(None, None, None), P(None, "dp", None)
    return jax.shard_map(
        step,
        mesh=mesh,
        in_specs=(P(("rep", "dp"), None, None, None),) * 3 + (all_of,) * 3 + (cut,) * 6,
        out_specs=(P("rep", None, None),) * 3 + (P("rep", "dp", None),) * 6,
        check_vma=False,
    )
```
